32 devices in a mesh: span: 8 (over z, y), wall: 4 (over x, core).
Axes of the slice: x: 2, y: 2, z: 4, core: 2. Of those that a mesh axis runs over, the one named last changes fastest.
Arguments:
- random_field: float32 [3, 2048, 16384], P(None, 'wall', 'span'), may hold values from -6 to 6
- half_widths: int32 [2048], replicated, may hold values from 1 to 256, as said below
- band_pads: int32 [32], replicated, may hold values from 1 to 256, as said below
- span_widths: int32 [32], replicated, may hold values from 1 to 64, as said below
- stresses: float32 [6, 2048], P(None, 'wall'), as said below
- mean_flow: float32 [2048], P('wall'), may hold values from 0.3 to 1.2
Outputs:
- velocity: float32 [3, 2048, 16384], P(None, 'wall', 'span')
The draws below stay inside these ranges and needn't reach their ends.
Inputs may be any that keep to these rules, and one draw needn't show every extreme that they name: `half_widths`: every row's value is at most the band_pads value of its band of 64 rows; some row reaches 256. `band_pads`: some band reaches 256. `span_widths`: some band reaches 64. `stresses`: each row's six entries form a positive definite tensor whose correlation coefficients are at most 0.4 in magnitude; the diagonal entries lie between 0.3 and 3.
All inputs are finite; a program needn't handle non-finite values.
Results may differ from the reference program's by a relative error of at most 0.0003.
Values sent between devices are 32-bit elements; how exact they have to be, the bound alone decides.
A program may use at most 192 MiB of HBM per device.

```python
import jax
import jax.numpy as jnp
from jax import lax

MAXW = 256
SPMAX = 64
BAND = 64
NY = 2048
NS = 16384


def wall_tables(key):
    base = jax.random.fold_in(key, 4711)
    first, second, third = jax.random.split(base, 3)
    band_total = NY // BAND
    band_pads = jax.random.randint(first, (band_total,), 1, MAXW + 1)
    chosen = jax.random.randint(second, (), 0, band_total)
    band_pads = jnp.where(jnp.arange(band_total) == chosen, MAXW, band_pads)
    raw_draw = jax.random.randint(third, (band_total * BAND,), 0, MAXW)
    halves = 1 + raw_draw % jnp.repeat(band_pads, BAND)
    halves = jnp.where(jnp.arange(band_total * BAND) == chosen * BAND, MAXW, halves)
    return (band_pads.astype(jnp.int32), halves.astype(jnp.int32))


def draw_half_widths(key, part):
    return wall_tables(key)[1]


def draw_band_pads(key, part):
    return wall_tables(key)[0]


def draw_span_widths(key, part):
    base = jax.random.fold_in(key, 919)
    first, second = jax.random.split(base)
    band_total = NY // BAND
    widths = jax.random.randint(first, (band_total,), 1, SPMAX + 1)
    chosen = jax.random.randint(second, (), 0, band_total)
    return jnp.where(jnp.arange(band_total) == chosen, SPMAX, widths).astype(jnp.int32)


def draw_stresses(key, part):
    base = jax.random.fold_in(key, 313)
    first, second = jax.random.split(base)
    logs = jax.random.uniform(first, (3, NY), jnp.float32, jnp.log(0.3), jnp.log(3.0))
    diagonal = jnp.exp(logs)
    correl = jax.random.uniform(second, (3, NY), jnp.float32, -0.4, 0.4)
    cross_uv = correl[0] * jnp.sqrt(diagonal[0] * diagonal[1])
    cross_uw = correl[1] * jnp.sqrt(diagonal[0] * diagonal[2])
    cross_vw = correl[2] * jnp.sqrt(diagonal[1] * diagonal[2])
    return jnp.stack([diagonal[0], diagonal[1], diagonal[2], cross_uv, cross_uw, cross_vw], axis=0).astype(jnp.float32)


def levels(rng, dims, pieces, least, top_value):
    level, own = 1.0, jax.random.fold_in(rng, 6)
    for position, shards_of in pieces:
        draws = jnp.exp(jax.random.uniform(jax.random.fold_in(own, position), (shards_of,), jnp.float32, least / len(pieces), top_value / len(pieces)))
        level = level * jnp.repeat(draws, dims[position] // shards_of).reshape([-1 if axis == position else 1 for axis in range(len(dims))])
    return level


def noise(rng, shape, scale, limit, cuts=(), held_as=jnp.bfloat16):
    factor_of = levels(rng, shape, cuts, -0.22, 0.18) if cuts else 1.0
    array = jax.random.normal(rng, shape, jnp.float32) * scale * factor_of
    return jnp.minimum(jnp.maximum(array, -limit), limit).astype(held_as)


def setup_inputs(seed: int = 0) -> dict:
    keys = jax.random.split(jax.random.key(seed), 7)
    return {
        "random_field": noise(keys[0], (3, NY, NS), 1.0, 6.0, ((1, 4), (2, 8)), jnp.float32),
        "half_widths": draw_half_widths(jax.random.fold_in(keys[6], 71), 0),
        "band_pads": draw_band_pads(jax.random.fold_in(keys[6], 71), 0),
        "span_widths": draw_span_widths(jax.random.fold_in(keys[6], 71), 0),
        "stresses": draw_stresses(jax.random.fold_in(keys[6], 71), 0),
        "mean_flow": jnp.clip(0.3 + 0.90000004 * jax.random.uniform(keys[5], (NY,), jnp.float32) ** levels(keys[5], (NY,), ((0, 4),), -0.2, 0.2), 0.3, 1.2),
    }


def wall_kernel(halves, pad_value):
    offsets = (jnp.arange(BAND + 2 * MAXW)[None, :] - MAXW - jnp.arange(BAND)[:, None]).astype(jnp.float32)
    spread = halves.astype(jnp.float32)[:, None]
    inside = jnp.abs(offsets) <= pad_value.astype(jnp.float32)
    coeffs = jnp.where(inside, jnp.exp(-jnp.pi * offsets * offsets / (2.0 * spread * spread)), jnp.float32(0.0))
    return coeffs / jnp.sqrt(lax.optimization_barrier(jnp.sum(coeffs * coeffs, axis=1, keepdims=True)))

def lund_apply(psi, stresses, mean_flow):
    lund_aa = jnp.sqrt(stresses[0])
    lund_ba = stresses[3] / lund_aa
    lund_bb = jnp.sqrt(stresses[1] - lund_ba * lund_ba)
    lund_ca = stresses[4] / lund_aa
    lund_cb = (stresses[5] - lund_ba * lund_ca) / lund_bb
    lund_cc = jnp.sqrt(stresses[2] - lund_ca * lund_ca - lund_cb * lund_cb)
    stream = mean_flow[:, None] + lund_aa[:, None] * psi[0]
    normal = lund_ba[:, None] * psi[0] + lund_bb[:, None] * psi[1]
    spanwise = lund_ca[:, None] * psi[0] + lund_cb[:, None] * psi[1] + lund_cc[:, None] * psi[2]
    return jnp.stack([stream, normal, spanwise], axis=0)

def reference(random_field, half_widths, band_pads, span_widths, stresses, mean_flow):
    channels, total_rows, total_cols = random_field.shape
    reach = 2 * SPMAX
    wrapped = jnp.concatenate([random_field[:, :, total_cols - reach:], random_field, random_field[:, :, :reach]], axis=2)
    row_widths = jnp.repeat(span_widths, BAND).astype(jnp.float32)
    offsets = (jnp.arange(2 * reach + 1) - reach).astype(jnp.float32)
    profile = jnp.where(jnp.abs(offsets)[:, None] <= 2.0 * row_widths[None, :], jnp.exp(-jnp.pi * offsets[:, None] ** 2 / (2.0 * row_widths[None, :] ** 2)), jnp.float32(0.0))
    profile = profile / jnp.sqrt(lax.optimization_barrier(jnp.sum(profile * profile, axis=0, keepdims=True)))

    def accumulate(shift_index, total):
        shift_index = jnp.asarray(shift_index).astype(jnp.int32)
        piece = lax.dynamic_slice_in_dim(wrapped, shift_index, total_cols, 2)
        weight = lax.dynamic_index_in_dim(profile, shift_index, 0, keepdims=False)
        return total + weight[None, :, None] * piece
    spanwise = lax.fori_loop(0, 2 * reach + 1, accumulate, jnp.zeros(random_field.shape, jnp.float32))
    extended = jnp.pad(spanwise, ((0, 0), (MAXW, MAXW), (0, 0)))

    def one_band(band_index):
        start = (band_index * BAND).astype(jnp.int32)
        window = lax.dynamic_slice_in_dim(extended, start, BAND + 2 * MAXW, 1)
        halves = lax.dynamic_slice_in_dim(half_widths, start, BAND, 0)
        pad_value = lax.dynamic_index_in_dim(band_pads, band_index.astype(jnp.int32), 0, keepdims=False)
        kernel = wall_kernel(halves, pad_value)
        return jnp.einsum('ij,cjs->cis', kernel, window, precision=lax.Precision.HIGHEST)
    blocks = lax.map(one_band, jnp.arange(total_rows // BAND).astype(jnp.int32))
    psi = jnp.moveaxis(blocks, 0, 1).reshape(channels, total_rows, total_cols)
    return lund_apply(psi, stresses, mean_flow)
```

```python
import functools

import jax
import jax.numpy as jnp
from jax import lax
from jax.experimental import pallas as pl
from jax.experimental.pallas import tpu as pltpu
from jax.sharding import PartitionSpec as P


MAXW = 256
SPMAX = 64
BAND = 64
REACH = 2 * SPMAX
TILE = 4 * SPMAX
HALF = TILE // 2
CHUNK = 2


def split(values):
    high = values.astype(jnp.bfloat16)
    low = (values - high.astype(jnp.float32)).astype(jnp.bfloat16)
    return high, low


def dot3(a, b):
    dot = functools.partial(jnp.dot, preferred_element_type=jnp.float32)
    return dot(a[0], b[0]) + (dot(a[0], b[1]) + dot(a[1], b[0]))


def span_tables(span_half):
    spread = span_half.astype(jnp.float32)[:, None, None]
    offsets = (jnp.arange(2 * REACH + 1) - REACH).astype(jnp.float32)[None, None, :]
    profile = jnp.where(
        jnp.abs(offsets) <= 2.0 * spread,
        jnp.exp(-jnp.pi * offsets * offsets / (2.0 * spread * spread)),
        jnp.float32(0.0),
    )
    scaling = 1.0 / jnp.sqrt(jnp.sum(profile * profile, axis=2, keepdims=True))
    shifts = (
        jnp.arange(TILE + 2 * REACH)[:, None] - REACH - jnp.arange(TILE)[None, :]
    ).astype(jnp.float32)[None]
    coeffs = jnp.where(
        jnp.abs(shifts) <= 2.0 * spread,
        jnp.exp(shifts * shifts * (-jnp.pi / (2.0 * spread * spread))),
        jnp.float32(0.0),
    )
    return coeffs * scaling


def wall_tables(halves, row_pads):
    offsets = (jnp.arange(3 * MAXW)[None, :] - MAXW - jnp.arange(MAXW)[:, None]).astype(
        jnp.float32
    )[None]
    spread = halves.astype(jnp.float32).reshape(-1, MAXW, 1)
    pads = row_pads.astype(jnp.float32).reshape(-1, MAXW, 1)
    coeffs = jnp.where(
        jnp.abs(offsets) <= pads,
        jnp.exp(offsets * offsets * (-jnp.pi / (2.0 * spread * spread))),
        jnp.float32(0.0),
    )
    return coeffs / jnp.sqrt(jnp.sum(coeffs * coeffs, axis=2, keepdims=True))


def span_body(runs, bands_half, *refs):
    pieces = sum(2 * (n + 1) for n in runs)
    halves, table, top, bottom = refs[:pieces], refs[pieces], refs[pieces + 1], refs[pieces + 2]
    band = pl.program_id(0)
    first = split(table[0, :TILE, :])
    second = split(table[0, TILE:, :])
    at = 0
    results = []
    for n in runs:
        tiles = []
        for t in range(n + 1):
            left = halves[at + 2 * t][...]
            right = halves[at + 2 * t + 1][...]
            joined = jnp.concatenate([left, right], axis=2)
            tiles.append(split(joined.reshape(3 * BAND, TILE)))
        at += 2 * (n + 1)
        low = tuple(jnp.concatenate([tiles[t][i] for t in range(n)], axis=0) for i in range(2))
        high = tuple(
            jnp.concatenate([tiles[t][i] for t in range(1, n + 1)], axis=0) for i in range(2)
        )
        made = dot3(low, first) + dot3(high, second)
        for t in range(n):
            results.append(made[t * 3 * BAND : (t + 1) * 3 * BAND].reshape(3, BAND, TILE))

    def store(ref):
        for i, value in enumerate(results):
            ref[:, :, i * TILE : (i + 1) * TILE] = value

    @pl.when(band < bands_half)
    def _():
        store(top)

    @pl.when(band >= bands_half)
    def _():
        store(bottom)


def span_chunk(pieces, runs, table):
    channels, rows, _ = pieces[0][0].shape
    bands = rows // BAND
    half = bands // 2
    width = sum(runs) * TILE
    in_specs = [
        pl.BlockSpec((channels, BAND, HALF), lambda b, c=col: (0, b, c)) for _, col in pieces
    ]
    in_specs.append(pl.BlockSpec((1, TILE + 2 * REACH, TILE), lambda b: (b, 0, 0)))
    shape = jax.ShapeDtypeStruct((channels, rows // 2, width), jnp.float32)
    return pl.pallas_call(
        functools.partial(span_body, runs, half),
        grid=(bands,),
        in_specs=in_specs,
        out_specs=[
            pl.BlockSpec((channels, BAND, width), lambda b: (0, jnp.minimum(b, half - 1), 0)),
            pl.BlockSpec((channels, BAND, width), lambda b: (0, jnp.maximum(b - half, 0), 0)),
        ],
        out_shape=[shape, shape],
        compiler_params=pltpu.CompilerParams(
            dimension_semantics=("arbitrary",), vmem_limit_bytes=48 << 20
        ),
        cost_estimate=pl.CostEstimate(
            flops=3 * 2 * channels * rows * width * 2 * TILE,
            bytes_accessed=4 * channels * rows * width * 2 + table.size * 4,
            transcendentals=0,
        ),
    )(*[array for array, _ in pieces], table)


def wall_body(low, top, bottom, high, table, factor, *rest):
    out = rest[-1]
    psi = []
    tables = [split(table[0]), split(table[1])]
    for c in range(3):
        parts = [split(ref[c]) for ref in (low, top, bottom, high)]
        blocks = []
        for h in range(2):
            window = tuple(
                jnp.concatenate([parts[h + k][i] for k in range(3)], axis=0) for i in range(2)
            )
            blocks.append(dot3(tables[h], window))
        psi.append(blocks)
    for h in range(2):
        at = slice(h * MAXW, (h + 1) * MAXW)
        a = [factor[at, i : i + 1] for i in range(7)]
        u, v, w = psi[0][h], psi[1][h], psi[2][h]
        out[0, at, :] = a[6] + a[0] * u
        out[1, at, :] = a[1] * u + a[2] * v
        out[2, at, :] = a[3] * u + a[4] * v + a[5] * w


def wall_chunk(low, top, bottom, high, table, factor, out, shape, first, stride):
    channels, rows, _ = shape
    count = top.shape[2] // TILE
    block = pl.BlockSpec((channels, MAXW, TILE), lambda i: (0, 0, i))
    in_specs = [
        block,
        block,
        block,
        block,
        pl.BlockSpec(table.shape, lambda i: (0, 0, 0)),
        pl.BlockSpec(factor.shape, lambda i: (0, 0)),
    ]
    operands = [low, top, bottom, high, table, factor]
    aliases = {}
    if out is not None:
        in_specs.append(pl.BlockSpec(memory_space=pl.ANY))
        aliases = {len(operands): 0}
        operands.append(out)
    return pl.pallas_call(
        wall_body,
        grid=(count,),
        in_specs=in_specs,
        out_specs=pl.BlockSpec((channels, rows, TILE), lambda i: (0, 0, first + stride * i)),
        out_shape=jax.ShapeDtypeStruct(shape, jnp.float32),
        input_output_aliases=aliases,
        compiler_params=pltpu.CompilerParams(
            dimension_semantics=("arbitrary",), vmem_limit_bytes=56 << 20
        ),
        cost_estimate=pl.CostEstimate(
            flops=3 * 2 * channels * rows * 3 * MAXW * count * TILE,
            bytes_accessed=4 * channels * rows * count * TILE * 3,
            transcendentals=0,
        ),
    )(*operands)


def lund_factor(stresses, mean_flow):
    aa = jnp.sqrt(stresses[0])
    ba = stresses[3] / aa
    bb = jnp.sqrt(stresses[1] - ba * ba)
    ca = stresses[4] / aa
    cb = (stresses[5] - ba * ca) / bb
    cc = jnp.sqrt(stresses[2] - ca * ca - cb * cb)
    return jnp.stack([aa, ba, bb, ca, cb, cc, mean_flow, mean_flow], axis=1)


def shift(value, axis, step, periodic):
    count = lax.axis_size(axis)
    pairs = [
        (i, (i + step) % count) for i in range(count) if periodic or 0 <= i + step < count
    ]
    return lax.ppermute(value, axis, pairs)


def shards(random_field, half_widths, band_pads, span_widths, stresses, mean_flow):
    shape = random_field.shape
    rows, cols = shape[1], shape[2]
    assert rows == 2 * MAXW and cols % TILE == 0
    tiles = cols // TILE
    first_row = lax.axis_index("wall") * rows
    first_band = first_row // BAND
    bands = rows // BAND

    from_left = shift(random_field[:, :, cols - REACH :], "span", 1, True)
    from_right = shift(random_field[:, :, :REACH], "span", -1, True)

    span_half = lax.dynamic_slice_in_dim(span_widths, first_band, bands, 0)
    table = span_tables(span_half)
    halves = lax.dynamic_slice_in_dim(half_widths, first_row, rows, 0)
    pads = jnp.repeat(lax.dynamic_slice_in_dim(band_pads, first_band, bands, 0), BAND)
    walls = wall_tables(halves, pads)
    factor = lund_factor(stresses, mean_flow)

    plan = []
    start = 1
    while start < tiles - 1:
        n = min(CHUNK, tiles - 1 - start)
        pieces = [(random_field, 2 * start - 1 + k) for k in range(2 * (n + 1))]
        plan.append((pieces, (n,), start, 1))
        start += n
    last = 2 * tiles
    edge = [(from_left, 0)] + [(random_field, k) for k in range(3)]
    edge += [(random_field, last - 3 + k) for k in range(3)] + [(from_right, 0)]
    plan.append((edge, (1, 1), 0, tiles - 1))

    sent = []
    for pieces, runs, first, stride in plan:
        top, bottom = span_chunk(pieces, runs, table)
        low = shift(bottom, "wall", 1, False)
        high = shift(top, "wall", -1, False)
        sent.append((low, top, bottom, high, first, stride))
    out = None
    for low, top, bottom, high, first, stride in sent:
        out = wall_chunk(low, top, bottom, high, walls, factor, out, shape, first, stride)
    return out


def solution(mesh):
    return jax.shard_map(
        shards,
        mesh=mesh,
        in_specs=(P(None, "wall", "span"), P(), P(), P(), P(None, "wall"), P("wall")),
        out_specs=P(None, "wall", "span"),
        check_vma=False,
    )
```
